32 devices in a mesh: dp: 2 (over y), ep: 16 (over z, x, core).
Axes of the slice: x: 2, y: 2, z: 4, core: 2. Of those that a mesh axis runs over, the one named last changes fastest.
Arguments:
- tokens: bfloat16 [16, 2, 1, 3584], P('ep', 'dp'), may hold values from -6 to 6
- gate_weights: bfloat16 [16, 2, 1, 8], P('ep', 'dp'), may hold values from 0.099609375 to 0.59765625
- expert_ids: int32 [16, 2, 1, 8], P('ep', 'dp'), may hold values from 0 to 15, all different within a row; in each aligned block of 2 rows (0 to 1, 2 to 3, ..., all dimensions but the last counted through in order) at most 2 rows name the same one
- gate_proj: bfloat16 [16, 3584, 2048], P('ep', None, 'dp'), may hold values from -0.09375 to 0.09375
- up_proj: bfloat16 [16, 3584, 2048], P('ep', None, 'dp'), may hold values from -0.09375 to 0.09375
- down_proj: bfloat16 [16, 2048, 3584], P('ep', 'dp'), may hold values from -0.125 to 0.125
Outputs:
- mixed: bfloat16 [16, 2, 1, 3584], P('ep', 'dp')
The draws below stay inside these ranges and needn't reach their ends.
Inputs may be any that keep to these rules, and one draw needn't show every extreme that they name: `expert_ids`: each token names 8 different experts. Among the 2 tokens of one index of the first dimension, no expert is named more than 2 times, a bound that some block reaches.
All inputs are finite; a program needn't handle non-finite values.
Results may differ from the reference program's by a relative error of at most 0.02.
Values may be sent and summed in bfloat16 or wider, within the bound.
A program may use at most 64 MiB of HBM per device.

```python
import math
import jax
import jax.numpy as jnp
import numpy as np
from jax import lax

D = 3584
FF = 2048
TOP = 8
TOK_DEV = 1
CAP = 2
EXPERTS = 16
N_DP = 2
N_EP = 16


def level_of(rng, shape, pieces, smallest, largest):
    factor_of = 1.0
    for dim, shards_of in pieces:
        steps = jax.random.uniform(jax.random.fold_in(jax.random.fold_in(rng, 6), dim), (shards_of,), jnp.float32, smallest / len(pieces), largest / len(pieces))
        factor_of = factor_of * jnp.repeat(jnp.exp(steps), shape[dim] // shards_of).reshape((-1,) + (1,) * (len(shape) - 1 - dim))
    return factor_of


def routed_block(own_key, own, number, rows, amount, top, most, lean):
    sequence = jax.random.permutation(own_key, amount)
    crowded, usual = portions_of(amount, rows * top, most, lean, True), portions_of(amount, rows * top, most, lean, False)
    places = jnp.arange(amount)

    def named(lengths, rotation):
        used = int((lengths > 0).sum())
        fixed = max(1, used // 4)
        passed = fixed + (places - fixed + rotation * (used - fixed)) % max(1, amount - fixed)
        return jnp.zeros((amount,), jnp.int32).at[sequence[jnp.where(places < fixed, places, passed)]].set(jnp.asarray(lengths, jnp.int32))

    lengths = jnp.where(number % 4 == 0, named(crowded, number // 4), named(usual, number - number // 4 - 1))
    mixed = jax.random.permutation(jax.random.fold_in(own, 3), amount)
    giver, receiver = mixed[0:amount // 2 * 2:2], mixed[1:amount // 2 * 2:2]
    margin = jnp.minimum(lengths[giver] - 1, most - lengths[receiver]) // 2
    margin = jnp.where((giver == sequence[0]) | (receiver == sequence[0]) | (lengths[receiver] == 0), 0, jnp.maximum(margin, 0))
    passed = jax.random.randint(jax.random.fold_in(own, 4), (amount // 2,), 0, 1 << 20) % (margin + 1)
    lengths = lengths.at[giver].add(-passed).at[receiver].add(passed)
    items = jnp.searchsorted(jnp.cumsum(lengths), jnp.arange(rows * top), side="right").astype(jnp.int32)
    listing = items.reshape(top, rows).T
    listing = listing[jax.random.permutation(jax.random.fold_in(own, 1), rows)]
    rotation = jax.random.randint(jax.random.fold_in(own, 2), (rows, 1), 0, top)
    return jnp.take_along_axis(listing, (jnp.arange(top)[None, :] + rotation) % top, axis=1)


def portions_of(number_of, total, reach, slope, full):
    loads = [(1 << 20) // math.isqrt(grade ** slope) + 1 for grade in range(1, number_of + 1)]
    largest = reach if full else min(reach, max(-(-total // number_of), total * loads[0] // sum(loads)))
    least = 1 if total - largest >= number_of - 1 else 0
    counts, rest = [largest] + [least] * (number_of - 1), total - largest - least * (number_of - 1)
    while rest > 0:
        candidates = [i for i in range(1, number_of) if counts[i] < largest] or [i for i in range(1, number_of) if counts[i] < reach]
        whole, budget = sum([loads[i] for i in candidates]), rest
        for i in candidates:
            addition = min(reach - counts[i], max(1, budget * loads[i] // whole), rest)
            counts[i] = counts[i] + addition
            rest = rest - addition
    return np.array(counts)


def scatter_about(key, dims, spread, limit, split=(), kind=jnp.bfloat16):
    factor_of = level_of(key, dims, split, -0.22, 0.18) if split else 1.0
    entries = jax.random.normal(key, dims, jnp.float32) * spread * factor_of
    return jnp.minimum(jnp.maximum(entries, -limit), limit).astype(kind)


def setup_inputs(seed: int = 0) -> dict:
    streams_of = jax.random.split(jax.random.key(seed), 7)
    tokens = scatter_about(streams_of[0], (N_EP, N_DP, TOK_DEV, D), 1.0, 6.0, ((0, 16), (1, 2)))
    gate_weights = jnp.clip(0.099609375 + 0.49804688 * jax.random.uniform(streams_of[1], (N_EP, N_DP, TOK_DEV, TOP), jnp.float32) ** level_of(streams_of[1], (N_EP, N_DP, TOK_DEV, TOP), ((0, 16), (1, 2)), -0.2, 0.2), 0.099609375, 0.59765625).astype(jnp.bfloat16)
    expert_ids_keys = jax.random.split(jax.random.fold_in(streams_of[2], 1), N_EP * N_DP * TOK_DEV // (N_DP * TOK_DEV))
    expert_ids_turns = jax.random.permutation(jax.random.fold_in(streams_of[2], 3), N_EP * N_DP * TOK_DEV // (N_DP * TOK_DEV))
    expert_ids = jax.vmap(lambda own, number: routed_block(jax.random.fold_in(streams_of[2], 2), own, number, N_DP * TOK_DEV, EXPERTS, TOP, CAP, 2))(expert_ids_keys, expert_ids_turns).reshape((N_EP, N_DP, TOK_DEV, TOP))
    gate_proj = scatter_about(streams_of[3], (EXPERTS, D, FF), D ** -0.5, 0.09375, ((0, 16), (2, 2)))
    up_proj = scatter_about(streams_of[4], (EXPERTS, D, FF), D ** -0.5, 0.09375, ((0, 16), (2, 2)))
    down_proj = scatter_about(streams_of[5], (EXPERTS, FF, D), FF ** -0.5, 0.125, ((0, 16), (1, 2)))
    return dict(tokens=tokens, gate_weights=gate_weights, expert_ids=expert_ids, gate_proj=gate_proj, up_proj=up_proj, down_proj=down_proj)


def placing(flat_ids, expert_count, capacity):
    labels = jnp.arange(expert_count, dtype=jnp.int32)
    onehot = (flat_ids[:, None] == labels[None, :]).astype(jnp.int32)
    earlier = jnp.cumsum(onehot, axis=0) - onehot
    slot_index = jnp.sum(earlier * onehot, axis=1).astype(jnp.int32)
    destination = (flat_ids * capacity + slot_index).astype(jnp.int32)
    targets = jnp.arange(expert_count * capacity, dtype=jnp.int32)
    return (destination[:, None] == targets[None, :]).astype(jnp.float32)


def expert_forward(operands):
    slot_rows, gate_mat, up_mat, down_mat = operands
    gate_act = jnp.dot(slot_rows, gate_mat, preferred_element_type=jnp.float32)
    up_act = jnp.dot(slot_rows, up_mat, preferred_element_type=jnp.float32)
    hidden = (jax.nn.silu(gate_act) * up_act).astype(jnp.bfloat16)
    return jnp.dot(hidden, down_mat, preferred_element_type=jnp.float32).astype(jnp.bfloat16)


def reference(tokens, gate_weights, expert_ids, gate_proj, up_proj, down_proj):
    column_total, group_count, token_count, feature_count = tokens.shape
    expert_count = gate_proj.shape[0]
    top_count = expert_ids.shape[3]
    capacity = CAP
    token_total = group_count * token_count
    slot_total = expert_count * capacity

    def place_column(column_ids):
        return placing(column_ids, expert_count, capacity)

    flat_ids = expert_ids.reshape(column_total, token_total * top_count).astype(jnp.int32)
    placed = jax.vmap(place_column)(flat_ids)
    selection = jnp.sum(placed.reshape(column_total, token_total, top_count, slot_total), axis=2)
    token_rows = tokens.reshape(column_total, token_total, feature_count).astype(jnp.float32)
    buffer = jnp.einsum("ctj,ctd->cjd", selection, token_rows, precision=lax.Precision.HIGHEST).astype(jnp.bfloat16)
    per_expert = buffer.reshape(column_total, expert_count, capacity, feature_count)
    per_expert = per_expert.transpose(1, 0, 2, 3).reshape(expert_count, column_total * capacity, feature_count)
    expert_out = lax.map(expert_forward, (per_expert, gate_proj, up_proj, down_proj))
    expert_out = expert_out.reshape(expert_count, column_total, capacity, feature_count)
    expert_out = expert_out.transpose(1, 0, 2, 3).reshape(column_total, slot_total, feature_count)
    weight_flat = gate_weights.reshape(column_total, token_total * top_count).astype(jnp.float32)
    weighted = jnp.sum((placed * weight_flat[:, :, None]).reshape(column_total, token_total, top_count, slot_total), axis=2)
    mixed = jnp.einsum("ctj,cjd->ctd", weighted, expert_out.astype(jnp.float32), precision=lax.Precision.HIGHEST)
    return mixed.astype(jnp.bfloat16).reshape(tokens.shape)
```

```python
import functools

import jax
import jax.numpy as jnp
from jax import lax
from jax.experimental import pallas as pl
from jax.experimental.pallas import tpu as pltpu
from jax.sharding import PartitionSpec as P


def placing(flat_ids, expert_count, capacity):
    labels = jnp.arange(expert_count, dtype=jnp.int32)
    onehot = (flat_ids[:, None] == labels[None, :]).astype(jnp.int32)
    earlier = jnp.cumsum(onehot, axis=0) - onehot
    slot_index = jnp.sum(earlier * onehot, axis=1)
    destination = flat_ids * capacity + slot_index
    targets = jnp.arange(expert_count * capacity, dtype=jnp.int32)
    return (destination[:, None] == targets[None, :]).astype(jnp.float32)


def body(tokens, gate_weights, expert_ids, gate_proj, up_proj, down_proj):
    group_count = lax.axis_size("dp")
    expert_count = lax.axis_size("ep")
    token_count = tokens.shape[2]
    feature_count = tokens.shape[3]
    top_count = expert_ids.shape[3]
    capacity = min(
        group_count * token_count, token_count * (group_count * top_count // expert_count + 1)
    )
    token_total = group_count * token_count
    slot_total = expert_count * capacity
    column_count = feature_count // group_count
    all_ids = lax.all_gather(expert_ids, "dp", axis=1, tiled=True)
    placed = placing(all_ids.reshape(-1), expert_count, capacity)
    selection = jnp.sum(placed.reshape(token_total, top_count, slot_total), axis=1)
    selection_t = selection.T.astype(jnp.bfloat16)
    token_rows, all_weights = (
        lax.all_gather(tokens, "dp", axis=1, tiled=True),
        lax.all_gather(gate_weights, "dp", axis=1, tiled=True),
    )
    buffer = jnp.dot(
        selection_t,
        token_rows.reshape(token_total, feature_count),
        preferred_element_type=jnp.float32,
    ).astype(jnp.bfloat16)
    received = lax.all_to_all(
        buffer.reshape(expert_count, capacity, feature_count),
        "ep",
        split_axis=0,
        concat_axis=0,
        tiled=True,
    )
    slot_rows = received.reshape(slot_total, feature_count)
    gate_act = jnp.dot(slot_rows, gate_proj[0], preferred_element_type=jnp.float32)
    up_act = jnp.dot(slot_rows, up_proj[0], preferred_element_type=jnp.float32)
    hidden = (jax.nn.silu(gate_act) * up_act).astype(jnp.bfloat16)
    down_mat = down_proj[0]
    summed_t = lax.psum_scatter(
        lax.dot_general(
            down_mat, hidden, (((0,), (1,)), ((), ())), preferred_element_type=jnp.float32
        ).astype(jnp.bfloat16),
        "dp",
        scatter_dimension=0,
        tiled=True,
    ).astype(jnp.float32)
    summed = summed_t.T.astype(jnp.bfloat16).reshape(expert_count, capacity, column_count)
    returned = lax.all_to_all(summed, "ep", split_axis=0, concat_axis=0, tiled=True)
    weight_flat = all_weights.reshape(-1).astype(jnp.float32)
    weighted = jnp.sum(
        (placed * weight_flat[:, None]).reshape(token_total, top_count, slot_total), axis=1
    )
    mixed = jnp.dot(
        weighted,
        returned.reshape(slot_total, column_count).astype(jnp.float32),
        precision=lax.Precision.HIGHEST,
    ).astype(jnp.bfloat16)
    own = lax.all_to_all(
        mixed.reshape(group_count, token_count, column_count),
        "dp",
        split_axis=0,
        concat_axis=2,
        tiled=True,
    )
    return own.reshape(1, 1, token_count, feature_count)


LANES = 128
MESH = pl.DeviceIdType.MESH


def kernel(
    groups,
    experts,
    pieces,
    tok_ref,
    weight_ref,
    ids_ref,
    gate_hbm,
    up_hbm,
    down_hbm,
    out_ref,
    gate_w,
    up_w,
    down_w,
    own32,
    own16,
    rows16,
    rows32,
    rows_mat,
    sent16,
    got16,
    gate_sem,
    up_sem,
    down_sem,
    tok_send,
    tok_recv,
    res_send,
    res_recv,
):
    total = groups * experts
    features, hidden_count = gate_hbm.shape
    blocks = features // LANES
    pitch = own32.shape[0]
    step = features // pieces

    gate_copies, up_copies, down_copies = [], [], []
    for p in range(pieces):
        part = pl.ds(p * step, step)
        gate_copies.append(pltpu.make_async_copy(gate_hbm.at[part], gate_w.at[part], gate_sem.at[p]))
        up_copies.append(pltpu.make_async_copy(up_hbm.at[part], up_w.at[part], up_sem.at[p]))
        down_copies.append(
            pltpu.make_async_copy(down_hbm.at[:, part], down_w.at[:, part], down_sem.at[p])
        )
    for p in range(pieces):
        gate_copies[p].start()
        up_copies[p].start()
    for p in range(pieces):
        down_copies[p].start()

    me = lax.axis_index("ep") * groups + lax.axis_index("dp")

    def place(flat):
        return (flat % groups, flat // groups)

    barrier = pltpu.get_barrier_semaphore()

    def greet(d, carry):
        pl.semaphore_signal(
            barrier, inc=1, device_id=place((me + d) % total), device_id_type=MESH
        )
        return carry

    lax.fori_loop(1, total, greet, 0)

    own32[...] = jnp.zeros_like(own32)
    for j in range(blocks):
        own32[j : j + 1, :] = tok_ref[:, j * LANES : (j + 1) * LANES].astype(jnp.float32)
    own16[...] = own32[...].astype(jnp.bfloat16)

    pl.semaphore_wait(barrier, total - 1)

    def token_copy(target, slot):
        return pltpu.make_async_remote_copy(
            src_ref=own16,
            dst_ref=rows16.at[slot],
            send_sem=tok_send.at[target],
            recv_sem=tok_recv.at[slot],
            device_id=place(target),
            device_id_type=MESH,
        )

    def send_token(d, carry):
        token_copy((me + d) % total, me).start()
        return carry

    lax.fori_loop(1, total, send_token, 0)
    rows16[me] = own16[...]

    def wait_token(d, carry):
        other = (me + d) % total
        token_copy(other, other).wait_recv()
        return carry

    lax.fori_loop(1, total, wait_token, 0)

    for t in range(total):
        rows32[t * pitch : (t + 1) * pitch, :] = rows16[t].astype(jnp.float32)
    for j in range(blocks):
        rows_mat[:, j * LANES : (j + 1) * LANES] = rows32[
            pl.ds(j, total, stride=pitch), :
        ].astype(jnp.bfloat16)

    gate_act = jnp.zeros((total, hidden_count), jnp.float32)
    up_act = jnp.zeros((total, hidden_count), jnp.float32)
    for p in range(pieces):
        part = slice(p * step, (p + 1) * step)
        left = rows_mat[:, part]
        gate_copies[p].wait()
        gate_act += jnp.dot(left, gate_w[part, :], preferred_element_type=jnp.float32)
        up_copies[p].wait()
        up_act += jnp.dot(left, up_w[part, :], preferred_element_type=jnp.float32)
    hidden = (gate_act / (1.0 + jnp.exp(-gate_act)) * up_act).astype(jnp.bfloat16)

    for p in range(pieces):
        down_copies[p].wait()
        result = jnp.dot(
            hidden, down_w[:, p * step : (p + 1) * step], preferred_element_type=jnp.float32
        )
        for j in range(step // LANES):
            rows32[pl.ds(p * (step // LANES) + j, total, stride=pitch), :] = result[
                :, j * LANES : (j + 1) * LANES
            ]
    for t in range(total):
        sent16[t] = rows32[t * pitch : (t + 1) * pitch, :].astype(jnp.bfloat16)

    def result_copy(target, slot):
        return pltpu.make_async_remote_copy(
            src_ref=sent16.at[target],
            dst_ref=got16.at[slot],
            send_sem=res_send.at[target],
            recv_sem=res_recv.at[slot],
            device_id=place(target),
            device_id_type=MESH,
        )

    def send_result(d, carry):
        result_copy((me + d) % total, me).start()
        return carry

    lax.fori_loop(1, total, send_result, 0)
    got16[me] = sent16[me]

    labels = lax.broadcasted_iota(jnp.int32, (experts, ids_ref.shape[1]), 0)
    chosen = jnp.where(ids_ref[...] == labels, weight_ref[...].astype(jnp.float32), 0.0)
    mix = jnp.broadcast_to(jnp.sum(chosen, axis=1, keepdims=True), (experts, LANES))

    def wait_result(d, carry):
        other = (me + d) % total
        result_copy(other, other).wait_recv()
        return carry

    lax.fori_loop(1, total, wait_result, 0)

    mixed = jnp.zeros((pitch, LANES), jnp.float32)
    for e in range(experts):
        both = got16[e * groups].astype(jnp.float32)
        for g in range(1, groups):
            both += got16[e * groups + g].astype(jnp.float32)
        mixed += mix[e : e + 1, :] * both
    for j in range(blocks):
        out_ref[:, j * LANES : (j + 1) * LANES] = mixed[j : j + 1, :].astype(jnp.bfloat16)

    def wait_sends(d, carry):
        other = (me + d) % total
        token_copy(other, me).wait_send()
        result_copy(other, me).wait_send()
        return carry

    lax.fori_loop(1, total, wait_sends, 0)


def small_body(tokens, gate_weights, expert_ids, gate_proj, up_proj, down_proj):
    groups = lax.axis_size("dp")
    experts = lax.axis_size("ep")
    total = groups * experts
    features = tokens.shape[3]
    top_count = expert_ids.shape[3]
    hidden_count = gate_proj.shape[2]
    blocks = features // LANES
    pitch = -(-blocks // 16) * 16
    pieces = max(p for p in (7, 4, 2, 1) if blocks % p == 0)
    vmem = pl.BlockSpec(memory_space=pltpu.VMEM)
    hbm = pl.BlockSpec(memory_space=pl.ANY)
    dma = pltpu.SemaphoreType.DMA
    out = pl.pallas_call(
        functools.partial(kernel, groups, experts, pieces),
        out_shape=jax.ShapeDtypeStruct((1, features), jnp.bfloat16),
        in_specs=[vmem, vmem, vmem, hbm, hbm, hbm],
        out_specs=vmem,
        scratch_shapes=[
            pltpu.VMEM((features, hidden_count), jnp.bfloat16),
            pltpu.VMEM((features, hidden_count), jnp.bfloat16),
            pltpu.VMEM((hidden_count, features), jnp.bfloat16),
            pltpu.VMEM((pitch, LANES), jnp.float32),
            pltpu.VMEM((pitch, LANES), jnp.bfloat16),
            pltpu.VMEM((total, pitch, LANES), jnp.bfloat16),
            pltpu.VMEM((total * pitch, LANES), jnp.float32),
            pltpu.VMEM((total, features), jnp.bfloat16),
            pltpu.VMEM((total, pitch, LANES), jnp.bfloat16),
            pltpu.VMEM((total, pitch, LANES), jnp.bfloat16),
            dma((pieces,)),
            dma((pieces,)),
            dma((pieces,)),
            dma((total,)),
            dma((total,)),
            dma((total,)),
            dma((total,)),
        ],
        compiler_params=pltpu.CompilerParams(collective_id=0, has_side_effects=True),
    )(
        tokens.reshape(1, features),
        gate_weights.reshape(1, top_count),
        expert_ids.reshape(1, top_count),
        gate_proj[0],
        up_proj[0],
        down_proj[0],
    )
    return out.reshape(1, 1, 1, features)


def layer(tokens, gate_weights, expert_ids, gate_proj, up_proj, down_proj):
    groups = lax.axis_size("dp")
    total = groups * lax.axis_size("ep")
    held = 3 * gate_proj.size * gate_proj.dtype.itemsize
    one_each = tokens.shape[2] == 1 and tokens.shape[3] % LANES == 0
    fits = total <= 64 and total % 16 == 0 and held <= 36 << 20
    few = groups <= groups * expert_ids.shape[3] // lax.axis_size("ep") + 1
    form = small_body if one_each and fits and few else body
    return form(tokens, gate_weights, expert_ids, gate_proj, up_proj, down_proj)


def solution(mesh):
    placed = (
        P("ep", "dp", None, None),
        P("ep", "dp", None, None),
        P("ep", "dp", None, None),
        P("ep", None, "dp"),
        P("ep", None, "dp"),
        P("ep", "dp", None),
    )
    return jax.shard_map(
        layer, mesh=mesh, in_specs=placed, out_specs=P("ep", "dp", None, None), check_vma=False
    )
```

```python
import functools

import jax
import jax.numpy as jnp
from jax import lax
from jax.experimental import pallas as pl
from jax.experimental.pallas import tpu as pltpu
from jax.sharding import PartitionSpec as P


def placing(flat_ids, expert_count, capacity):
    labels = jnp.arange(expert_count, dtype=jnp.int32)
    onehot = (flat_ids[:, None] == labels[None, :]).astype(jnp.int32)
    earlier = jnp.cumsum(onehot, axis=0) - onehot
    slot_index = jnp.sum(earlier * onehot, axis=1)
    destination = flat_ids * capacity + slot_index
    targets = jnp.arange(expert_count * capacity, dtype=jnp.int32)
    return (destination[:, None] == targets[None, :]).astype(jnp.float32)


def body(tokens, gate_weights, expert_ids, gate_proj, up_proj, down_proj):
    group_count = lax.axis_size("dp")
    expert_count = lax.axis_size("ep")
    token_count = tokens.shape[2]
    feature_count = tokens.shape[3]
    top_count = expert_ids.shape[3]
    capacity = min(
        group_count * token_count, token_count * (group_count * top_count // expert_count + 1)
    )
    token_total = group_count * token_count
    slot_total = expert_count * capacity
    column_count = feature_count // group_count
    all_ids = lax.all_gather(expert_ids, "dp", axis=1, tiled=True)
    placed = placing(all_ids.reshape(-1), expert_count, capacity)
    selection = jnp.sum(placed.reshape(token_total, top_count, slot_total), axis=1)
    selection_t = selection.T.astype(jnp.bfloat16)
    token_rows, all_weights = (
        lax.all_gather(tokens, "dp", axis=1, tiled=True),
        lax.all_gather(gate_weights, "dp", axis=1, tiled=True),
    )
    buffer = jnp.dot(
        selection_t,
        token_rows.reshape(token_total, feature_count),
        preferred_element_type=jnp.float32,
    ).astype(jnp.bfloat16)
    received = lax.all_to_all(
        buffer.reshape(expert_count, capacity, feature_count),
        "ep",
        split_axis=0,
        concat_axis=0,
        tiled=True,
    )
    slot_rows = received.reshape(slot_total, feature_count)
    gate_act = jnp.dot(slot_rows, gate_proj[0], preferred_element_type=jnp.float32)
    up_act = jnp.dot(slot_rows, up_proj[0], preferred_element_type=jnp.float32)
    hidden = (jax.nn.silu(gate_act) * up_act).astype(jnp.bfloat16)
    down_mat = down_proj[0]
    summed_t = lax.psum_scatter(
        lax.dot_general(
            down_mat, hidden, (((0,), (1,)), ((), ())), preferred_element_type=jnp.float32
        ).astype(jnp.bfloat16),
        "dp",
        scatter_dimension=0,
        tiled=True,
    ).astype(jnp.float32)
    summed = summed_t.T.astype(jnp.bfloat16).reshape(expert_count, capacity, column_count)
    returned = lax.all_to_all(summed, "ep", split_axis=0, concat_axis=0, tiled=True)
    weight_flat = all_weights.reshape(-1).astype(jnp.float32)
    weighted = jnp.sum(
        (placed * weight_flat[:, None]).reshape(token_total, top_count, slot_total), axis=1
    )
    mixed = jnp.dot(
        weighted,
        returned.reshape(slot_total, column_count).astype(jnp.float32),
        precision=lax.Precision.HIGHEST,
    ).astype(jnp.bfloat16)
    own = lax.all_to_all(
        mixed.reshape(group_count, token_count, column_count),
        "dp",
        split_axis=0,
        concat_axis=2,
        tiled=True,
    )
    return own.reshape(1, 1, token_count, feature_count)


LANES = 128
BAND = 16
MESH = pl.DeviceIdType.MESH


def kernel(
    groups,
    experts,
    pieces,
    tok_ref,
    weight_ref,
    ids_ref,
    gate_hbm,
    up_hbm,
    down_hbm,
    out_ref,
    gate_w,
    up_w,
    down_w,
    own32,
    own16,
    rows16,
    rows32,
    rows_mat,
    sent16,
    pair16,
    halved16,
    got16,
    gate_sem,
    up_sem,
    down_sem,
    line_send,
    plane_send,
    share_send,
    tok_recv,
    pair_send,
    pair_recv,
    res_send,
    res_recv,
):
    total = groups * experts
    features, hidden_count = gate_hbm.shape
    blocks = features // LANES
    pitch = own32.shape[0]
    step = features // pieces
    cores, across = 2, 2
    lines = experts // (cores * across)
    chips = total // cores
    bands = pitch // BAND

    gate_copies, up_copies, down_copies = [], [], []
    for p in range(pieces):
        part = pl.ds(p * step, step)
        gate_copies.append(pltpu.make_async_copy(gate_hbm.at[part], gate_w.at[part], gate_sem.at[p]))
        up_copies.append(pltpu.make_async_copy(up_hbm.at[part], up_w.at[part], up_sem.at[p]))
        down_copies.append(
            pltpu.make_async_copy(down_hbm.at[:, part], down_w.at[:, part], down_sem.at[p])
        )

    my_group = lax.axis_index("dp")
    my_expert = lax.axis_index("ep")
    core = my_expert % cores
    my_across = (my_expert // cores) % across
    line = my_expert // (cores * across)

    def flat(z, x, c, g):
        return ((z * across + x) * cores + c) * groups + g

    def where(slot):
        return (slot % groups, slot // groups)

    def chip_of(slot):
        return slot // (groups * cores) * groups + slot % groups

    me = flat(line, my_across, core, my_group)
    partner = flat(line, my_across, 1 - core, my_group)
    on_line = [flat((line + k) % lines, my_across, core, my_group) for k in range(lines)]
    near = [
        ((my_across + i) % across, (my_group + j) % groups)
        for i in range(across)
        for j in range(groups)
        if i or j
    ]
    in_plane = [flat(line, x, core, g) for x, g in near]

    barrier = pltpu.get_barrier_semaphore()
    friends = on_line[1:] + in_plane + [partner]
    for slot in friends:
        pl.semaphore_signal(barrier, inc=1, device_id=where(slot), device_id_type=MESH)

    for p in range(pieces):
        gate_copies[p].start()
        up_copies[p].start()
    for p in range(pieces):
        down_copies[p].start()

    own32[...] = jnp.zeros_like(own32)
    for j in range(blocks):
        own32[j : j + 1, :] = tok_ref[:, j * LANES : (j + 1) * LANES].astype(jnp.float32)
    lane = lax.broadcasted_iota(jnp.int32, (1, LANES), 1)
    mix = jnp.zeros((1, LANES), jnp.float32)
    for k in range(ids_ref.shape[1]):
        mix += jnp.where(
            lane == ids_ref[:, k : k + 1], weight_ref[:, k : k + 1].astype(jnp.float32), 0.0
        )
    own32[blocks : blocks + 1, :] = mix
    own16[...] = own32[...].astype(jnp.bfloat16)

    pl.semaphore_wait(barrier, len(friends))

    def token_copy(source, slot, target, send_sem):
        return pltpu.make_async_remote_copy(
            src_ref=source,
            dst_ref=rows16.at[slot],
            send_sem=send_sem,
            recv_sem=tok_recv.at[slot],
            device_id=where(target),
            device_id_type=MESH,
        )

    sends = []

    def send_token(source, slot, target, send_sem):
        copy = token_copy(source, slot, target, send_sem)
        copy.start()
        sends.append(copy)

    def wait_token(slot):
        token_copy(own16, slot, slot, line_send.at[0]).wait_recv()

    for k in range(1, lines):
        send_token(own16, me, on_line[k], line_send.at[k])
    for q, target in enumerate(in_plane):
        send_token(own16, me, target, plane_send.at[q])
    send_token(own16, me, partner, share_send.at[me])
    rows16[me] = own16[...]

    def reach(k):
        return [flat((line + k) % lines, x, core, g) for x, g in near]

    order = sorted(range(1, lines), key=lambda k: min(k, lines - k))
    for slot in reach(0):
        wait_token(slot)
        send_token(rows16.at[slot], slot, partner, share_send.at[slot])
    for k in order:
        wait_token(on_line[k])
        for q, target in enumerate(in_plane):
            send_token(
                rows16.at[on_line[k]], on_line[k], target, plane_send.at[k * len(near) + q]
            )
        send_token(rows16.at[on_line[k]], on_line[k], partner, share_send.at[on_line[k]])
    for k in order:
        for slot in reach(k):
            wait_token(slot)
            send_token(rows16.at[slot], slot, partner, share_send.at[slot])
    for k in range(lines):
        for x in range(across):
            for g in range(groups):
                wait_token(flat((line + k) % lines, x, 1 - core, g))

    for t in range(total):
        rows32[t * pitch : (t + 1) * pitch, :] = rows16[t].astype(jnp.float32)
    for j in range(blocks):
        rows_mat[:, j * LANES : (j + 1) * LANES] = rows32[
            pl.ds(j, total, stride=pitch), :
        ].astype(jnp.bfloat16)
    mixes = rows32[pl.ds(blocks, total, stride=pitch), :]
    labels = lax.broadcasted_iota(jnp.int32, (total, LANES), 1)
    scale = jnp.sum(jnp.where(labels == my_expert, mixes, 0.0), axis=1, keepdims=True)

    gate_act = jnp.zeros((total, hidden_count), jnp.float32)
    up_act = jnp.zeros((total, hidden_count), jnp.float32)
    for p in range(pieces):
        part = slice(p * step, (p + 1) * step)
        left = rows_mat[:, part]
        gate_copies[p].wait()
        gate_act += jnp.dot(left, gate_w[part, :], preferred_element_type=jnp.float32)
        up_copies[p].wait()
        up_act += jnp.dot(left, up_w[part, :], preferred_element_type=jnp.float32)
    hidden = (gate_act / (1.0 + jnp.exp(-gate_act)) * up_act).astype(jnp.bfloat16)

    def pair_copy(b):
        rows = pl.ds(b * BAND, BAND)
        return pltpu.make_async_remote_copy(
            src_ref=sent16.at[:, 1 - core, :, rows],
            dst_ref=pair16.at[:, :, rows],
            send_sem=pair_send.at[b],
            recv_sem=pair_recv.at[b],
            device_id=where(partner),
            device_id_type=MESH,
        )

    my_chip = chip_of(me)

    def result_copy(target, b, place):
        rows = pl.ds(b * BAND, BAND)
        return pltpu.make_async_remote_copy(
            src_ref=halved16.at[chip_of(target), rows],
            dst_ref=got16.at[place, rows],
            send_sem=res_send.at[chip_of(target), b],
            recv_sem=res_recv.at[place, b],
            device_id=where(target),
            device_id_type=MESH,
        )

    def other_chip(d):
        h = (my_chip + d) % chips
        return (h // groups * cores + core) * groups + h % groups

    def pass_on(b):
        rows = slice(b * BAND, (b + 1) * BAND)
        pair_copy(b).wait_recv()
        for h in range(chips):
            halved16[h, rows] = (
                sent16[h // groups, core, h % groups, rows].astype(jnp.float32)
                + pair16[h // groups, h % groups, rows].astype(jnp.float32)
            ).astype(jnp.bfloat16)

        def send_result(d, carry):
            result_copy(other_chip(d), b, my_chip).start()
            return carry

        lax.fori_loop(1, chips, send_result, 0)
        got16[my_chip, rows] = halved16[my_chip, rows]

    flushed = 0
    for p in range(pieces):
        down_copies[p].wait()
        result = scale * jnp.dot(
            hidden, down_w[:, p * step : (p + 1) * step], preferred_element_type=jnp.float32
        )
        for j in range(step // LANES):
            rows32[pl.ds(p * (step // LANES) + j, total, stride=pitch), :] = result[
                :, j * LANES : (j + 1) * LANES
            ]
        ready = (p + 1) * (step // LANES)
        while flushed < bands and ready >= min((flushed + 1) * BAND, blocks):
            low = flushed * BAND
            for t in range(total):
                sent16[t // (groups * cores), t // groups % cores, t % groups, low : low + BAND] = (
                    rows32[t * pitch + low : t * pitch + low + BAND, :].astype(jnp.bfloat16)
                )
            pair_copy(flushed).start()
            flushed += 1
    for b in range(bands):
        pass_on(b)

    for b in range(bands):

        def wait_result(d, carry):
            slot = other_chip(d)
            result_copy(slot, b, chip_of(slot)).wait_recv()
            return carry

        lax.fori_loop(1, chips, wait_result, 0)
        rows = slice(b * BAND, (b + 1) * BAND)
        mixed = got16[0, rows].astype(jnp.float32)
        for h in range(1, chips):
            mixed += got16[h, rows].astype(jnp.float32)
        for j in range(b * BAND, min((b + 1) * BAND, blocks)):
            out_ref[:, j * LANES : (j + 1) * LANES] = mixed[
                j - b * BAND : j - b * BAND + 1, :
            ].astype(jnp.bfloat16)

    for copy in sends:
        copy.wait_send()
    for b in range(bands):
        pair_copy(b).wait_send()

        def wait_sends(d, carry):
            result_copy(other_chip(d), b, my_chip).wait_send()
            return carry

        lax.fori_loop(1, chips, wait_sends, 0)


def small_body(tokens, gate_weights, expert_ids, gate_proj, up_proj, down_proj):
    groups = lax.axis_size("dp")
    experts = lax.axis_size("ep")
    total = groups * experts
    features = tokens.shape[3]
    top_count = expert_ids.shape[3]
    hidden_count = gate_proj.shape[2]
    blocks = features // LANES
    pitch = -(-(blocks + 1) // BAND) * BAND
    pieces = max(p for p in (7, 4, 2, 1) if blocks % p == 0)
    vmem = pl.BlockSpec(memory_space=pltpu.VMEM)
    hbm = pl.BlockSpec(memory_space=pl.ANY)
    dma = pltpu.SemaphoreType.DMA
    out = pl.pallas_call(
        functools.partial(kernel, groups, experts, pieces),
        out_shape=jax.ShapeDtypeStruct((1, features), jnp.bfloat16),
        in_specs=[vmem, vmem, vmem, hbm, hbm, hbm],
        out_specs=vmem,
        scratch_shapes=[
            pltpu.VMEM((features, hidden_count), jnp.bfloat16),
            pltpu.VMEM((features, hidden_count), jnp.bfloat16),
            pltpu.VMEM((hidden_count, features), jnp.bfloat16),
            pltpu.VMEM((pitch, LANES), jnp.float32),
            pltpu.VMEM((pitch, LANES), jnp.bfloat16),
            pltpu.VMEM((total, pitch, LANES), jnp.bfloat16),
            pltpu.VMEM((total * pitch, LANES), jnp.float32),
            pltpu.VMEM((total, features), jnp.bfloat16),
            pltpu.VMEM((experts // 2, 2, groups, pitch, LANES), jnp.bfloat16),
            pltpu.VMEM((experts // 2, groups, pitch, LANES), jnp.bfloat16),
            pltpu.VMEM((total // 2, pitch, LANES), jnp.bfloat16),
            pltpu.VMEM((total // 2, pitch, LANES), jnp.bfloat16),
            dma((pieces,)),
            dma((pieces,)),
            dma((pieces,)),
            dma((experts // 4,)),
            dma((experts // 4 * (2 * groups - 1),)),
            dma((total,)),
            dma((total,)),
            dma((pitch // BAND,)),
            dma((pitch // BAND,)),
            dma((total // 2, pitch // BAND)),
            dma((total // 2, pitch // BAND)),
        ],
        compiler_params=pltpu.CompilerParams(collective_id=0, has_side_effects=True),
    )(
        tokens.reshape(1, features),
        gate_weights.reshape(1, top_count),
        expert_ids.reshape(1, top_count),
        gate_proj[0],
        up_proj[0],
        down_proj[0],
    )
    return out.reshape(1, 1, 1, features)


def layer(tokens, gate_weights, expert_ids, gate_proj, up_proj, down_proj):
    groups = lax.axis_size("dp")
    total = groups * lax.axis_size("ep")
    held = 3 * gate_proj.size * gate_proj.dtype.itemsize
    one_each = tokens.shape[2] == 1 and tokens.shape[3] % LANES == 0
    fits = total <= 64 and total % 16 == 0 and lax.axis_size("ep") % 4 == 0 and held <= 36 << 20
    few = groups <= groups * expert_ids.shape[3] // lax.axis_size("ep") + 1
    form = small_body if one_each and fits and few else body
    return form(tokens, gate_weights, expert_ids, gate_proj, up_proj, down_proj)


def solution(mesh):
    placed = (
        P("ep", "dp", None, None),
        P("ep", "dp", None, None),
        P("ep", "dp", None, None),
        P("ep", None, "dp"),
        P("ep", None, "dp"),
        P("ep", "dp", None),
    )
    return jax.shard_map(
        layer, mesh=mesh, in_specs=placed, out_specs=P("ep", "dp", None, None), check_vma=False
    )
```
